32 devices in a mesh: tok: 8 (over y, x, core), layer: 4 (over z).
Axes of the slice: x: 2, y: 2, z: 4, core: 2. Of those that a mesh axis runs over, the one named last changes fastest.
Arguments:
- activations: bfloat16 [4, 896, 5120], P(None, ('tok', 'layer')), may hold values from -9 to 9
- pos_weight: bfloat16 [4, 48, 5120], P('layer', None, 'tok'), may hold values from -1 to 1
- depth_weight: bfloat16 [4, 128, 5120], P('layer', None, 'tok'), may hold values from -0.01953125 to 0.01953125
- tags: int32 [896], P(('tok', 'layer')), may hold values from 0 to 47
- depths: int32 [896], P(('tok', 'layer')), may hold values from 2 to 14
- counts: int32 [32], P(('tok', 'layer')), may hold values from 1 to 28, 560 in all
Outputs:
- pos_grad: float32 [4, 48, 5120], P('layer', None, 'tok')
- depth_grad: float32 [4, 128, 5120], P('layer', None, 'tok')
The draws below stay inside these ranges and needn't reach their ends.
Inputs may be any that keep to these rules, and one draw needn't show every extreme that they name: counts[d] is the number of live slots among device d's 28 slots, which are its first ones; the largest count equals 28.
All inputs are finite; a program needn't handle non-finite values.
Results may differ from the reference program's by a relative error of at most 0.0042.
Values may be sent and summed in bfloat16 or wider, within the bound.
No kernel may reach another device: no remote copies, remote signals or barrier semaphores. Data moves between devices by JAX's collectives and lax.ppermute only.
A program may use at most 64 MiB of HBM per device.

```python
import math
import jax
import jax.numpy as jnp
import numpy as np
from jax import lax

D = 5120
TAGS = 48
RANK = 128
TOK_DEV = 28
LAYERS = 4
TOKENS = 896
DEVICES = 32


def probe_table(key):
    base = jax.random.normal(jax.random.fold_in(key, 11), (LAYERS, TAGS, D), jnp.float32)
    table = jnp.clip(base, -6.0, 6.0) / jnp.sqrt(jnp.float32(D))
    return table


def draw_pos_weight(key, part):
    return probe_table(key).astype(jnp.bfloat16)


def draw_activations(key, part):
    noise = jax.random.normal(jax.random.fold_in(key, 12), (LAYERS, TOKENS, D), jnp.float32)
    rows = jnp.clip(noise, -6.0, 6.0)
    return rows.astype(jnp.bfloat16)


def plant(entries, own_key, low, high):
    shape = entries.shape
    place = [jax.random.randint(jax.random.fold_in(own_key, axis), (), 0, shape[axis]) for axis in range(len(shape))]
    entries = entries.at[tuple(place)].set(low)
    longest = shape.index(max(shape))
    place[longest] = (place[longest] + 1) % shape[longest]
    return entries.at[tuple(place)].set(high)


def block_scale(key, dims, cuts, least, high):
    loudness = 1.0
    for axis_at, shards_of in cuts:
        heights = jax.random.uniform(jax.random.fold_in(jax.random.fold_in(key, 6), axis_at), (shards_of,), jnp.float32, least / len(cuts), high / len(cuts))
        loudness = loudness * jnp.repeat(jnp.exp(heights), dims[axis_at] // shards_of).reshape((-1,) + (1,) * (len(dims) - 1 - axis_at))
    return loudness


def split_up(count, total, most, lean):
    weights = [(1 << 20) // math.isqrt(standing ** lean) + 1 for standing in range(2, count + 1)]
    surplus, holding = total - most - (count - 1), [1] * (count - 1)
    while surplus > 0:
        candidates = [i for i in range(count - 1) if holding[i] < most]
        mass, remaining = sum([weights[i] for i in candidates]), surplus
        for i in candidates:
            extra = min(most - holding[i], max(1, remaining * weights[i] // mass), surplus)
            holding[i] = holding[i] + extra
            surplus = surplus - extra
    return np.array([most] + holding)


def ragged(own_key, number_of, total, limit, lean):
    if number_of == 2:
        one = jax.random.randint(own_key, (), max(1, total - limit), min(limit, total - 1) + 1)
        return jnp.stack([one, total - one])
    tallies = jnp.asarray(split_up(number_of, total, limit, lean), jnp.int32)
    couples = (number_of - 1) // 2
    giver, receiver = tallies[1:1 + 2 * couples:2], tallies[2:2 + 2 * couples:2]
    slack = jnp.minimum(giver - 1, limit - receiver)
    passed = jax.random.randint(jax.random.fold_in(own_key, 1), (couples,), 0, 1 << 20) % (slack + 1)
    tallies = tallies.at[1:1 + 2 * couples:2].set(giver - passed).at[2:2 + 2 * couples:2].set(receiver + passed)
    return tallies[jax.random.permutation(jax.random.fold_in(own_key, 2), number_of)]


def centred(rng, extent, width, bound, cuts=(), held_as=jnp.bfloat16):
    result = jax.random.normal(rng, extent, jnp.float32) * width
    if len(cuts) > 0:
        result = block_scale(rng, extent, cuts, -0.22, 0.18) * result
    return jnp.clip(result, min=-bound, max=bound).astype(held_as)


def setup_inputs(seed: int = 0) -> dict:
    splits = jax.random.split(jax.random.key(seed), 7)
    activations = draw_activations(jax.random.fold_in(splits[6], 71), 0)
    pos_weight = draw_pos_weight(jax.random.fold_in(splits[6], 71), 0)
    depth_weight = centred(splits[2], (LAYERS, RANK, D), (16 * D) ** -0.5, 0.01953125, ((0, 4), (2, 8)))
    tags = plant(jax.random.randint(splits[3], (TOKENS,), 0, TAGS), jax.random.fold_in(splits[3], 1), 0, TAGS - 1).astype(jnp.int32)
    depths = plant(jax.random.randint(splits[4], (TOKENS,), 2, 15), jax.random.fold_in(splits[4], 1), 2, 14).astype(jnp.int32)
    counts = ragged(splits[5], DEVICES, DEVICES * TOK_DEV * 5 // 8, TOK_DEV, 2).astype(jnp.int32)
    return {"activations": activations, "pos_weight": pos_weight, "depth_weight": depth_weight, "tags": tags, "depths": depths, "counts": counts}


def layer_grads(layer_rows, pos_layer, depth_layer, tags, depths, counts):
    logits = jnp.dot(layer_rows, pos_layer.T, preferred_element_type=jnp.float32)
    hidden = jnp.dot(layer_rows, depth_layer.T, preferred_element_type=jnp.float32)
    slot_index = jnp.arange(TOKENS, dtype=jnp.int32)
    position = slot_index % TOK_DEV
    block_index = slot_index // TOK_DEV
    block_count = counts[block_index]
    live = position < block_count
    token_scale = jnp.where(live, 1.0 / block_count.astype(jnp.float32), jnp.float32(0.0))
    top = jnp.max(logits, axis=1, keepdims=True)
    expo = jnp.exp(logits - top)
    probabilities = expo / jnp.sum(expo, axis=1, keepdims=True)
    onehot = (tags[:, None] == jnp.arange(TAGS, dtype=jnp.int32)[None, :]).astype(jnp.float32)
    g_pos = (probabilities - onehot) * token_scale[:, None]
    predicted = jnp.sum(hidden * hidden, axis=1)
    residual = predicted - depths.astype(jnp.float32)
    g_depth = hidden * (residual * token_scale)[:, None]
    joined = jnp.concatenate([g_pos, g_depth], axis=1).astype(jnp.bfloat16)
    grad = lax.dot_general(joined, layer_rows, (((0,), (0,)), ((), ())), preferred_element_type=jnp.float32)
    return grad[:TAGS], grad[TAGS:]


def reference(activations, pos_weight, depth_weight, tags, depths, counts):
    def one_layer(items):
        return layer_grads(items[0], items[1], items[2], tags, depths, counts)

    pos_grad, depth_grad = lax.map(one_layer, (activations, pos_weight, depth_weight))
    return pos_grad, depth_grad
```

```python
import functools

import jax
import jax.numpy as jnp
from jax import lax
from jax.experimental import pallas as pl
from jax.experimental.pallas import tpu as pltpu
from jax.sharding import PartitionSpec as P


LANES = 128


def contract(left, right):
    return lax.dot_general(
        left, right, (((1,), (1,)), ((), ())), preferred_element_type=jnp.float32
    )


def steps(count):
    width = count.bit_length() - 2
    chips = sorted(range(1, count // 2), key=lambda c: (-c.bit_count(), c))
    mirrored = [sum((c >> n & 1) << (width - 1 - n) for n in range(width)) for c in chips]
    return [(0, 0)] + [(2 * a, 2 * b) for a, b in zip(chips, mirrored)]


def peer(tok, step):
    first, second = step
    if isinstance(tok, int):
        return tok ^ (second if tok % 2 else first)
    return tok ^ jnp.where(tok % 2 == 0, first, second)


def swap(value, step):
    pairs = [(i, peer(i, step)) for i in range(lax.axis_size("tok"))]
    return lax.ppermute(value, "tok", pairs)


def gray(i):
    return i ^ (i >> 1)


def ungray(i, count):
    total = i
    for n in range(1, count.bit_length()):
        total = total ^ (i >> n)
    return total


def ring_shifts(count):
    return [1, count - 1] + list(range(2, count - 1))


def ring_target(i, shift, count):
    return gray((ungray(i, count) + shift) % count)


def spans(slots, pieces):
    base = slots // 8 * 8
    return [(p, 0, base) for p in range(pieces)] + [
        (p, base, slots) for p in range(pieces) if base < slots
    ]


def tile_rows(slots, lo, hi, tile):
    base = slots // 8 * 8
    start = tile // 2 * 2 * slots
    if lo < base:
        start += tile % 2 * base
    else:
        start += 2 * base + tile % 2 * (slots - base)
    return slice(start, start + hi - lo)


def round_up(value, step):
    return -(-value // step) * step


def pick_rows(held, target, out, slots, layers, tiles):
    base = slots // 8 * 8
    for t in tiles:
        rows = held[t, pl.ds(target, slots, stride=layers), :].astype(out.dtype)
        out[tile_rows(slots, 0, base, t), :] = rows[:base]
        if base < slots:
            out[tile_rows(slots, base, slots, t), :] = rows[base:]


def first_kernel(me, act, pos, depth, out, held, probe, raw, act_sems, sems, *, slots, layers):
    width = act.shape[2]
    parts = act_sems.shape[0]
    step = width // parts
    tag_count = pos.shape[1]
    loads = [
        pltpu.make_async_copy(
            act.at[:, :, pl.ds(n * step, step)], raw.at[:, :, pl.ds(n * step, step)], act_sems.at[n]
        )
        for n in range(parts)
    ]
    others = [
        pltpu.make_async_copy(pos.at[0], probe.at[:tag_count], sems.at[0]),
        pltpu.make_async_copy(depth.at[0], probe.at[tag_count:], sems.at[1]),
    ]
    for copy in loads + others:
        copy.start()
    target = ring_target(me[0], ring_shifts(layers)[0], layers)
    for n in range(parts):
        loads[n].wait()
        tiles = range(n * step // LANES, (n + 1) * step // LANES)
        for t in tiles:
            for s in range(slots):
                held[t, s * layers : (s + 1) * layers, :] = raw[
                    s, :, t * LANES : (t + 1) * LANES
                ].astype(jnp.float32)
        pick_rows(held, target, out, slots, layers, tiles)
    for copy in others:
        copy.wait()


def rest_kernel(me, held, *outs, slots, layers):
    targets = [me[0]] + [ring_target(me[0], s, layers) for s in ring_shifts(layers)[1:]]
    for target, out in zip(targets, outs):
        pick_rows(held, target, out, slots, layers, range(held.shape[0]))


def share_kernel(me, rows, probe, *outs, peers):
    grads, cols = probe.shape
    piece = outs[0].shape[0] - cols // LANES * grads
    for step, out in zip(peers, outs):
        out[:piece, :] = rows[pl.ds(chip_start(me[0], step, piece), piece), :]
        for t in range(cols // LANES):
            out[piece + t * grads : piece + (t + 1) * grads, :] = probe[
                :, t * LANES : (t + 1) * LANES
            ]


def cut_kernel(me, *refs, pieces, peers):
    parts, outs = refs[:pieces], refs[pieces:]
    piece = outs[0].shape[0] // pieces
    for step, out in zip(peers, outs):
        start = chip_start(me[0], step, piece)
        for n, part in enumerate(parts):
            out[n * piece : (n + 1) * piece, :] = part[pl.ds(start, piece), :]


def chip_start(tok, step, piece):
    return pl.multiple_of((peer(tok, step) // 2) * piece, 8)


def score_kernel(me, *refs, pieces, blocks, send, slots, tags, rank, peers):
    parts = refs[:pieces]
    probes = refs[pieces : pieces + len(blocks)]
    tokens = refs[pieces + len(blocks) : 2 * pieces + len(blocks)]
    outs, rows = refs[2 * pieces + len(blocks) : -1], refs[-1]
    grads = tags + rank
    tiles = rows.shape[1] // LANES
    tok_tiles = tiles // len(blocks)
    cols = tok_tiles * LANES
    piece = 2 * tok_tiles * slots
    order = spans(slots, pieces)
    at, facts = 0, []
    for p, lo, hi in order:
        for t in range(tiles):
            rows[at : at + hi - lo, t * LANES : (t + 1) * LANES] = parts[p][
                tile_rows(slots, lo, hi, t), :
            ]
        facts.append(tokens[p][:, lo:hi])
        at += hi - lo
    fact = jnp.concatenate(facts, axis=1)
    scores = None
    for (step, flip), block in zip(blocks, probes):
        spot = pl.ds(pl.multiple_of(peer(me[0] ^ flip, step) * cols, LANES), cols)
        probe = jnp.concatenate(
            [block[piece + t * grads : piece + (t + 1) * grads, :] for t in range(tok_tiles)], axis=1
        )
        part = contract(probe, rows[:, spot])
        scores = part if scores is None else scores + part
    logits, hidden = scores[:tags], scores[tags:]
    tag_row, depth_row, count_row, place = fact[0:1], fact[1:2], fact[2:3], fact[3:4]
    scale = jnp.where(place < count_row, 1.0 / count_row.astype(jnp.float32), jnp.float32(0.0))
    top = jnp.max(logits, axis=0, keepdims=True)
    expo = jnp.exp(logits - top)
    probabilities = expo / jnp.sum(expo, axis=0, keepdims=True)
    tag_at = lax.broadcasted_iota(jnp.int32, logits.shape, 0)
    onehot = (tag_at == tag_row).astype(jnp.float32)
    g_pos = (probabilities - onehot) * scale
    predicted = jnp.sum(hidden * hidden, axis=0, keepdims=True)
    g_depth = hidden * ((predicted - depth_row.astype(jnp.float32)) * scale)
    joined = jnp.concatenate([g_pos, g_depth], axis=0)
    folds = LANES // joined.shape[1]
    height = outs[0].shape[0] - piece
    if height * folds > grads:
        filler = jnp.zeros((height * folds - grads, joined.shape[1]), jnp.float32)
        joined = jnp.concatenate([joined, filler], axis=0)
    joined = jnp.concatenate([joined[n * height : (n + 1) * height] for n in range(folds)], axis=1)
    if joined.shape[1] < LANES:
        filler = jnp.zeros((height, LANES - joined.shape[1]), jnp.float32)
        joined = jnp.concatenate([joined, filler], axis=1)
    joined = joined.astype(jnp.bfloat16)
    for step, out in zip(peers, outs):
        out[:piece, :] = parts[send][pl.ds(chip_start(me[0], step, piece), piece), :]
        out[piece:, :] = joined


def fold_height(grads, tokens):
    folds = LANES // tokens
    return grads if folds == 1 else round_up(-(-grads // folds), 16)


def grad_kernel(me, *refs, chips, slots, layers):
    sets = [refs[n * chips : (n + 1) * chips] for n in range(layers)]
    other, left, right = refs[layers * chips :]
    grads, cols = other.shape
    tiles = 2 * cols // LANES
    piece = tiles * slots
    first = (layers - 1) * slots
    second = round_up(first, 8)
    folds = LANES // slots
    for c in range(chips):
        head = sets[1][c][piece:, :].astype(jnp.float32)
        tail = sets[-1][c][piece:, :].astype(jnp.float32)
        tail = jnp.concatenate([tail[:, n * slots : (n + 1) * slots] for n in range(folds)], axis=0)
        both = [head[:, :second], tail[:grads]]
        if second + slots < LANES:
            both.append(jnp.zeros((grads, LANES - second - slots), jnp.float32))
        at = c * LANES
        left[:, at : at + LANES] = jnp.concatenate(both, axis=1).astype(left.dtype)
        gaps = []
        for start, members in ((0, range(layers - 1)), (second, range(layers - 1, layers))):
            at = c * LANES + start
            for p, lo, hi in spans(slots, len(members)):
                for t in range(tiles):
                    right[at : at + hi - lo, t * LANES : (t + 1) * LANES] = sets[members[p]][c][
                        tile_rows(slots, lo, hi, t), :
                    ]
                at += hi - lo
            gaps.append((at, c * LANES + (second if start == 0 else LANES)))
        for lo, hi in gaps:
            if lo < hi:
                right[lo:hi, :] = jnp.zeros((hi - lo, 2 * cols), right.dtype)
    other[...] = half_grad(left, right, 1 - me[0] % 2, cols).astype(other.dtype)


def half_grad(left, right, half, cols):
    spot = pl.ds(pl.multiple_of(half * cols, LANES), cols)
    return jnp.dot(left[...], right[:, spot], preferred_element_type=jnp.float32)


def mine_kernel(me, left, right, mine):
    mine[...] = half_grad(left, right, me[0] % 2, mine.shape[1])


def join_kernel(mine, other, pos_out, depth_out):
    tags = pos_out.shape[1]
    pos_out[0] = mine[:tags] + other[:tags].astype(jnp.float32)
    depth_out[0] = mine[tags:] + other[tags:].astype(jnp.float32)


def call(vmem, kernel, outs, scratch, scalars, *values, spaces=()):
    local = pl.BlockSpec(memory_space=pltpu.VMEM)
    specs = [pl.BlockSpec(memory_space=pltpu.SMEM)] * len(scalars)
    specs += [pl.BlockSpec(memory_space=s) for s in spaces]
    specs += [local] * (len(values) - len(spaces))
    return pl.pallas_call(
        kernel,
        out_shape=outs,
        in_specs=specs,
        out_specs=[local] * len(outs),
        scratch_shapes=scratch,
        compiler_params=pltpu.CompilerParams(vmem_limit_bytes=vmem << 20),
    )(*scalars, *values)


def fast(activations, pos_weight, depth_weight, tags, depths, counts):
    layer_count, tok_count = lax.axis_size("layer"), lax.axis_size("tok")
    tag_count, cols = pos_weight.shape[1:]
    rank = depth_weight.shape[1]
    slots = tags.shape[0]
    layers, _, width = activations.shape
    bf16, f32, i32 = jnp.bfloat16, jnp.float32, jnp.int32
    shape = jax.ShapeDtypeStruct
    grads = tag_count + rank
    layer_at = lax.axis_index("layer").astype(i32)[None]
    tok_at = lax.axis_index("tok").astype(i32)[None]
    peers = steps(tok_count)
    piece = 2 * cols // LANES * slots

    def exchange(values):
        return [values[0]] + [swap(v, step) for step, v in zip(peers[1:], values[1:])]

    message = shape((width // LANES * slots, LANES), bf16)
    held_shape = (width // LANES, slots * layers, LANES)
    shifts = ring_shifts(layer_count)

    def along(value, shift):
        pairs = [(i, ring_target(i, shift, layer_count)) for i in range(layer_count)]
        return lax.ppermute(value, "layer", pairs)

    head, held, probe = call(
        12, functools.partial(first_kernel, slots=slots, layers=layers),
        [message, shape(held_shape, f32), shape((grads, cols), bf16)],
        [
            pltpu.VMEM((slots, layers, width), bf16),
            pltpu.SemaphoreType.DMA((4,)),
            pltpu.SemaphoreType.DMA((2,)),
        ],
        [layer_at],
        *[
            pltpu.with_memory_space_constraint(v, pltpu.HBM)
            for v in (jnp.transpose(activations, (1, 0, 2)), pos_weight, depth_weight)
        ],
        spaces=[pltpu.HBM] * 3,
    )
    own, *others = call(
        4, functools.partial(rest_kernel, slots=slots, layers=layers),
        [message] * (layers - 1), [], [layer_at], held,
    )
    pieces = [own] + [along(v, shift) for v, shift in zip([head] + others, shifts)]
    fact = jnp.stack([tags, depths, jnp.broadcast_to(counts, tags.shape), jnp.arange(slots, dtype=i32)])
    facts = [fact] + [along(fact, shift) for shift in shifts]
    shares = call(
        4, functools.partial(share_kernel, peers=peers),
        [shape((piece + cols // LANES * grads, LANES), bf16)] * len(peers),
        [], [tok_at], own, probe,
    )
    shares = exchange(shares)
    probes = shares + [swap(v, (1, 1)) for v in shares]
    blocks = [(step, 0) for step in peers] + [(step, 1) for step in peers]
    early = [
        exchange(
            call(
                4, functools.partial(cut_kernel, pieces=1, peers=peers),
                [shape((piece, LANES), bf16)] * len(peers), [], [tok_at], pieces[n],
            ),
        )
        for n in range(2, layers - 1)
    ]

    def score(members, send):
        outs = call(
            12,
            functools.partial(
                score_kernel, pieces=len(members), blocks=blocks, send=send, slots=slots,
                tags=tag_count, rank=rank, peers=peers,
            ),
            [shape((piece + fold_height(grads, len(members) * slots), LANES), bf16)] * len(peers),
            [pltpu.VMEM((len(members) * slots, width), bf16)],
            [tok_at], *[pieces[n] for n in members], *probes, *[facts[n] for n in members],
        )
        return exchange(outs)

    middle = score(range(layers - 1), 1)
    late = score([layers - 1], 0)
    other, left, right = call(
        8,
        functools.partial(grad_kernel, chips=len(peers), slots=slots, layers=layer_count),
        [
            shape((grads, cols), bf16),
            shape((grads, len(peers) * LANES), bf16),
            shape((len(peers) * LANES, 2 * cols), bf16),
        ],
        [], [tok_at], *shares, *middle, *[v for part in early for v in part], *late,
    )
    other = swap(other, (1, 1))
    (mine,) = call(4, mine_kernel, [shape((grads, cols), f32)], [], [tok_at], left, right)
    return call(
        4, join_kernel,
        [shape((1, tag_count, cols), f32), shape((1, rank, cols), f32)], [], [], mine, other,
    )


def general(activations, pos_weight, depth_weight, tags, depths, counts):
    tag_count = pos_weight.shape[1]
    slots = tags.shape[0]
    rows = lax.all_to_all(activations, "layer", split_axis=0, concat_axis=1, tiled=True)[0]
    probe = jnp.concatenate([pos_weight[0], depth_weight[0]], axis=0)
    probe = lax.all_gather(probe, "tok", axis=1, tiled=True)
    scores = contract(rows, probe)
    logits, hidden = scores[:, :tag_count], scores[:, tag_count:]
    facts = jnp.stack([tags, depths, jnp.broadcast_to(counts, tags.shape)])
    tag_row, depth_row, block_count = lax.all_gather(facts, "layer", axis=1, tiled=True)
    live = jnp.arange(rows.shape[0], dtype=jnp.int32) % slots < block_count
    scale = jnp.where(live, 1.0 / block_count.astype(jnp.float32), jnp.float32(0.0))
    expo = jnp.exp(logits - jnp.max(logits, axis=1, keepdims=True))
    probabilities = expo / jnp.sum(expo, axis=1, keepdims=True)
    onehot = (tag_row[:, None] == jnp.arange(tag_count, dtype=jnp.int32)[None, :]).astype(jnp.float32)
    g_pos = (probabilities - onehot) * scale[:, None]
    predicted = jnp.sum(hidden * hidden, axis=1)
    g_depth = hidden * ((predicted - depth_row.astype(jnp.float32)) * scale)[:, None]
    joined = jnp.concatenate([g_pos, g_depth], axis=1).astype(jnp.bfloat16)
    share = lax.dot_general(
        joined, rows, (((0,), (0,)), ((), ())), preferred_element_type=jnp.float32
    )
    summed = lax.psum_scatter(share, "tok", scatter_dimension=1, tiled=True)
    return summed[None, :tag_count], summed[None, tag_count:]


def fits(layer_count, tok_count, activations, pos_weight, depth_weight):
    layers, slots, width = activations.shape
    cols = pos_weight.shape[2]
    grads = pos_weight.shape[1] + depth_weight.shape[1]
    return (
        layers == layer_count
        and layers >= 4
        and layers & (layers - 1) == 0
        and tok_count >= 4
        and tok_count & (tok_count - 1) == 0
        and cols % LANES == 0
        and width == cols * tok_count
        and slots % 4 == 0
        and slots >= 8
        and round_up((layers - 1) * slots, 8) + slots <= LANES
        and grads % 16 == 0
        and pos_weight.shape[1] % 16 == 0
    )


def local(activations, pos_weight, depth_weight, tags, depths, counts):
    sizes = lax.axis_size("layer"), lax.axis_size("tok")
    if fits(*sizes, activations, pos_weight, depth_weight):
        return fast(activations, pos_weight, depth_weight, tags, depths, counts)
    return general(activations, pos_weight, depth_weight, tags, depths, counts)


def solution(mesh):
    in_specs = (
        P(None, ("tok", "layer"), None),
        P("layer", None, "tok"),
        P("layer", None, "tok"),
        P(("tok", "layer")),
        P(("tok", "layer")),
        P(("tok", "layer")),
    )
    out_specs = (P("layer", None, "tok"), P("layer", None, "tok"))

    return jax.shard_map(local, mesh=mesh, in_specs=in_specs, out_specs=out_specs, check_vma=False)
```

```python
import functools

import jax
import jax.numpy as jnp
from jax import lax
from jax.experimental import pallas as pl
from jax.experimental.pallas import tpu as pltpu
from jax.sharding import PartitionSpec as P


LANES = 128


def contract(left, right):
    return lax.dot_general(
        left, right, (((1,), (1,)), ((), ())), preferred_element_type=jnp.float32
    )


def steps(count):
    width = count.bit_length() - 2
    chips = sorted(range(1, count // 2), key=lambda c: (-c.bit_count(), c))
    mirrored = [sum((c >> n & 1) << (width - 1 - n) for n in range(width)) for c in chips]
    return [(0, 0)] + [(2 * a, 2 * b) for a, b in zip(chips, mirrored)]


def peer(tok, step):
    first, second = step
    if isinstance(tok, int):
        return tok ^ (second if tok % 2 else first)
    return tok ^ jnp.where(tok % 2 == 0, first, second)


def swap(value, step):
    pairs = [(i, peer(i, step)) for i in range(lax.axis_size("tok"))]
    return lax.ppermute(value, "tok", pairs)


def gray(i):
    return i ^ (i >> 1)


def ungray(i, count):
    total = i
    for n in range(1, count.bit_length()):
        total = total ^ (i >> n)
    return total


def ring_shifts(count):
    return [1, count - 1] + list(range(2, count - 1))


def ring_target(i, shift, count):
    return gray((ungray(i, count) + shift) % count)


def spans(slots, pieces):
    base = slots // 8 * 8
    return [(p, 0, base) for p in range(pieces)] + [
        (p, base, slots) for p in range(pieces) if base < slots
    ]


def tile_rows(slots, lo, hi, tile):
    base = slots // 8 * 8
    start = tile // 2 * 2 * slots
    if lo < base:
        start += tile % 2 * base
    else:
        start += 2 * base + tile % 2 * (slots - base)
    return slice(start, start + hi - lo)


def round_up(value, step):
    return -(-value // step) * step


def pick_rows(held, target, out, slots, layers, tiles):
    base = slots // 8 * 8
    for t in tiles:
        rows = held[t, pl.ds(target, slots, stride=layers), :].astype(out.dtype)
        out[tile_rows(slots, 0, base, t), :] = rows[:base]
        if base < slots:
            out[tile_rows(slots, base, slots, t), :] = rows[base:]


def first_kernel(me, act, pos, depth, out, held, probe, raw, act_sems, sems, *, slots, layers):
    width = act.shape[2]
    parts = act_sems.shape[0]
    step = width // parts
    tag_count = pos.shape[1]
    loads = [
        pltpu.make_async_copy(
            act.at[:, :, pl.ds(n * step, step)], raw.at[:, :, pl.ds(n * step, step)], act_sems.at[n]
        )
        for n in range(parts)
    ]
    others = [
        pltpu.make_async_copy(pos.at[0], probe.at[:tag_count], sems.at[0]),
        pltpu.make_async_copy(depth.at[0], probe.at[tag_count:], sems.at[1]),
    ]
    for copy in loads + others:
        copy.start()
    target = ring_target(me[0], ring_shifts(layers)[0], layers)
    for n in range(parts):
        loads[n].wait()
        tiles = range(n * step // LANES, (n + 1) * step // LANES)
        for t in tiles:
            for s in range(slots):
                held[t, s * layers : (s + 1) * layers, :] = raw[
                    s, :, t * LANES : (t + 1) * LANES
                ].astype(jnp.float32)
        pick_rows(held, target, out, slots, layers, tiles)
    for copy in others:
        copy.wait()


def rest_kernel(me, held, *outs, slots, layers):
    targets = [me[0]] + [ring_target(me[0], s, layers) for s in ring_shifts(layers)[1:]]
    for target, out in zip(targets, outs):
        pick_rows(held, target, out, slots, layers, range(held.shape[0]))


def share_kernel(me, rows, probe, *outs, peers):
    grads, cols = probe.shape
    piece = outs[0].shape[0] - cols // LANES * grads
    for step, out in zip(peers, outs):
        out[:piece, :] = rows[pl.ds(chip_start(me[0], step, piece), piece), :]
        for t in range(cols // LANES):
            out[piece + t * grads : piece + (t + 1) * grads, :] = probe[
                :, t * LANES : (t + 1) * LANES
            ]


def cut_kernel(me, *refs, pieces, peers):
    parts, outs = refs[:pieces], refs[pieces:]
    piece = outs[0].shape[0] // pieces
    for step, out in zip(peers, outs):
        start = chip_start(me[0], step, piece)
        for n, part in enumerate(parts):
            out[n * piece : (n + 1) * piece, :] = part[pl.ds(start, piece), :]


def chip_start(tok, step, piece):
    return pl.multiple_of((peer(tok, step) // 2) * piece, 8)


def score_kernel(me, *refs, pieces, blocks, send, slots, tags, rank, peers):
    parts = refs[:pieces]
    probes = refs[pieces : pieces + len(blocks)]
    tokens = refs[pieces + len(blocks) : 2 * pieces + len(blocks)]
    outs, rows = refs[2 * pieces + len(blocks) : -1], refs[-1]
    grads = tags + rank
    tiles = rows.shape[1] // LANES
    tok_tiles = tiles // len(blocks)
    cols = tok_tiles * LANES
    piece = 2 * tok_tiles * slots
    order = spans(slots, pieces)
    at, facts = 0, []
    for p, lo, hi in order:
        for t in range(tiles):
            rows[at : at + hi - lo, t * LANES : (t + 1) * LANES] = parts[p][
                tile_rows(slots, lo, hi, t), :
            ]
        facts.append(tokens[p][:, lo:hi])
        at += hi - lo
    fact = jnp.concatenate(facts, axis=1)
    scores = None
    spots = [
        pl.ds(pl.multiple_of(peer(me[0] ^ flip, step) * cols, LANES), cols) for step, flip in blocks
    ]
    for n in range(0, len(blocks), 4):
        members = range(n, min(n + 4, len(blocks)))
        probe = jnp.concatenate(
            [
                probes[m][piece + t * grads : piece + (t + 1) * grads, :]
                for m in members
                for t in range(tok_tiles)
            ],
            axis=1,
        )
        part = contract(probe, jnp.concatenate([rows[:, spots[m]] for m in members], axis=1))
        scores = part if scores is None else scores + part
    logits, hidden = scores[:tags], scores[tags:]
    tag_row, depth_row, count_row, place = fact[0:1], fact[1:2], fact[2:3], fact[3:4]
    scale = jnp.where(place < count_row, 1.0 / count_row.astype(jnp.float32), jnp.float32(0.0))
    top = jnp.max(logits, axis=0, keepdims=True)
    expo = jnp.exp(logits - top)
    probabilities = expo / jnp.sum(expo, axis=0, keepdims=True)
    tag_at = lax.broadcasted_iota(jnp.int32, logits.shape, 0)
    onehot = (tag_at == tag_row).astype(jnp.float32)
    g_pos = (probabilities - onehot) * scale
    predicted = jnp.sum(hidden * hidden, axis=0, keepdims=True)
    g_depth = hidden * ((predicted - depth_row.astype(jnp.float32)) * scale)
    joined = jnp.concatenate([g_pos, g_depth], axis=0)
    folds = LANES // joined.shape[1]
    height = outs[0].shape[0] - piece
    if height * folds > grads:
        filler = jnp.zeros((height * folds - grads, joined.shape[1]), jnp.float32)
        joined = jnp.concatenate([joined, filler], axis=0)
    joined = jnp.concatenate([joined[n * height : (n + 1) * height] for n in range(folds)], axis=1)
    if joined.shape[1] < LANES:
        filler = jnp.zeros((height, LANES - joined.shape[1]), jnp.float32)
        joined = jnp.concatenate([joined, filler], axis=1)
    joined = joined.astype(jnp.bfloat16)
    for step, out in zip(peers, outs):
        out[:piece, :] = parts[send][pl.ds(chip_start(me[0], step, piece), piece), :]
        out[piece:, :] = joined


def fold_height(grads, tokens):
    folds = LANES // tokens
    return grads if folds == 1 else round_up(-(-grads // folds), 16)


def gather_rows(right, at, sources, slots, tiles):
    for p, lo, hi in spans(slots, len(sources)):
        for t in range(tiles):
            right[at : at + hi - lo, t * LANES : (t + 1) * LANES] = sources[p][
                tile_rows(slots, lo, hi, t), :
            ]
        at += hi - lo
    return at


def stage_kernel(me, *refs, chips, slots, sets):
    messages = [refs[n * chips : (n + 1) * chips] for n in range(sets)]
    mine, other, left, right = refs[sets * chips :]
    cols = mine.shape[1]
    tiles = 2 * cols // LANES
    for c in range(chips):
        at, stop = c * LANES, (c + 1) * LANES
        left[:, at:stop] = messages[1][c][tiles * slots :, :]
        at = gather_rows(right, at, [part[c] for part in messages], slots, tiles)
        if at < stop:
            right[at:stop, :] = jnp.zeros((stop - at, 2 * cols), right.dtype)
    core = me[0] % 2
    mine[...] = half_grad(left, right, core, cols)
    other[...] = half_grad(left, right, 1 - core, cols)


def grad_kernel(me, *refs, chips, slots):
    lates, so_far = refs[:chips], refs[chips]
    other, left, right = refs[chips + 1 :]
    grads, cols = other.shape
    tiles = 2 * cols // LANES
    pad = right.shape[0] // chips
    folds = LANES // slots
    parts = []
    for c in range(chips):
        tail = lates[c][tiles * slots :, :].astype(jnp.float32)
        tail = jnp.concatenate([tail[:, n * slots : (n + 1) * slots] for n in range(folds)], axis=0)
        parts.append(tail[:grads])
        at, stop = c * pad, (c + 1) * pad
        if slots < pad:
            parts.append(jnp.zeros((grads, pad - slots), jnp.float32))
        at = gather_rows(right, at, [lates[c]], slots, tiles)
        if at < stop:
            right[at:stop, :] = jnp.zeros((stop - at, 2 * cols), right.dtype)
    left[...] = jnp.concatenate(parts, axis=1).astype(left.dtype)
    half = half_grad(left, right, 1 - me[0] % 2, cols)
    other[...] = (so_far[...] + half).astype(other.dtype)


def half_grad(left, right, half, cols):
    spot = pl.ds(pl.multiple_of(half * cols, LANES), cols)
    return jnp.dot(left[...], right[:, spot], preferred_element_type=jnp.float32)


def mine_kernel(me, left, right, so_far, mine):
    mine[...] = so_far[...] + half_grad(left, right, me[0] % 2, mine.shape[1])


def join_kernel(mine, other, pos_out, depth_out):
    tags = pos_out.shape[1]
    pos_out[0] = mine[:tags] + other[:tags].astype(jnp.float32)
    depth_out[0] = mine[tags:] + other[tags:].astype(jnp.float32)


def call(vmem, kernel, outs, scratch, scalars, *values, spaces=()):
    local = pl.BlockSpec(memory_space=pltpu.VMEM)
    specs = [pl.BlockSpec(memory_space=pltpu.SMEM)] * len(scalars)
    specs += [pl.BlockSpec(memory_space=s) for s in spaces]
    specs += [local] * (len(values) - len(spaces))
    return pl.pallas_call(
        kernel,
        out_shape=outs,
        in_specs=specs,
        out_specs=[local] * len(outs),
        scratch_shapes=scratch,
        compiler_params=pltpu.CompilerParams(vmem_limit_bytes=vmem << 20),
    )(*scalars, *values)


def fast(activations, pos_weight, depth_weight, tags, depths, counts):
    layer_count, tok_count = lax.axis_size("layer"), lax.axis_size("tok")
    tag_count, cols = pos_weight.shape[1:]
    rank = depth_weight.shape[1]
    slots = tags.shape[0]
    layers, _, width = activations.shape
    bf16, f32, i32 = jnp.bfloat16, jnp.float32, jnp.int32
    shape = jax.ShapeDtypeStruct
    grads = tag_count + rank
    layer_at = lax.axis_index("layer").astype(i32)[None]
    tok_at = lax.axis_index("tok").astype(i32)[None]
    peers = steps(tok_count)
    piece = 2 * cols // LANES * slots

    def exchange(values):
        return [values[0]] + [swap(v, step) for step, v in zip(peers[1:], values[1:])]

    message = shape((width // LANES * slots, LANES), bf16)
    held_shape = (width // LANES, slots * layers, LANES)
    shifts = ring_shifts(layer_count)

    def along(value, shift):
        pairs = [(i, ring_target(i, shift, layer_count)) for i in range(layer_count)]
        return lax.ppermute(value, "layer", pairs)

    head, held, probe = call(
        12, functools.partial(first_kernel, slots=slots, layers=layers),
        [message, shape(held_shape, f32), shape((grads, cols), bf16)],
        [
            pltpu.VMEM((slots, layers, width), bf16),
            pltpu.SemaphoreType.DMA((4,)),
            pltpu.SemaphoreType.DMA((2,)),
        ],
        [layer_at],
        *[
            pltpu.with_memory_space_constraint(v, pltpu.HBM)
            for v in (jnp.transpose(activations, (1, 0, 2)), pos_weight, depth_weight)
        ],
        spaces=[pltpu.HBM] * 3,
    )
    own, *others = call(
        4, functools.partial(rest_kernel, slots=slots, layers=layers),
        [message] * (layers - 1), [], [layer_at], held,
    )
    pieces = [own] + [along(v, shift) for v, shift in zip([head] + others, shifts)]
    fact = jnp.stack([tags, depths, jnp.broadcast_to(counts, tags.shape), jnp.arange(slots, dtype=i32)])
    facts = [fact] + [along(fact, shift) for shift in shifts]
    shares = call(
        4, functools.partial(share_kernel, peers=peers),
        [shape((piece + cols // LANES * grads, LANES), bf16)] * len(peers),
        [], [tok_at], own, probe,
    )
    shares = exchange(shares)
    probes = shares + [swap(v, (1, 1)) for v in shares]
    blocks = [(step, 0) for step in peers] + [(step, 1) for step in peers]
    early = [
        exchange(
            call(
                4, functools.partial(cut_kernel, pieces=1, peers=peers),
                [shape((piece, LANES), bf16)] * len(peers), [], [tok_at], pieces[n],
            ),
        )
        for n in range(2, layers - 1)
    ]

    def score(members, send):
        outs = call(
            12,
            functools.partial(
                score_kernel, pieces=len(members), blocks=blocks, send=send, slots=slots,
                tags=tag_count, rank=rank, peers=peers,
            ),
            [shape((piece + fold_height(grads, len(members) * slots), LANES), bf16)] * len(peers),
            [pltpu.VMEM((len(members) * slots, width), bf16)],
            [tok_at], *[pieces[n] for n in members], *probes, *[facts[n] for n in members],
        )
        return exchange(outs)

    middle = score(range(layers - 1), 1)
    late = score([layers - 1], 0)
    part = shape((grads, cols), f32)
    count = len(peers)
    mine, other = call(
        8, functools.partial(stage_kernel, chips=count, slots=slots, sets=layers - 1),
        [part, part],
        [pltpu.VMEM((grads, count * LANES), bf16), pltpu.VMEM((count * LANES, 2 * cols), bf16)],
        [tok_at], *shares, *middle, *[v for values in early for v in values],
    )
    depth = count * round_up(slots, 16)
    other, left, right = call(
        8, functools.partial(grad_kernel, chips=count, slots=slots),
        [shape((grads, cols), bf16), shape((grads, depth), bf16), shape((depth, 2 * cols), bf16)],
        [], [tok_at], *late, other,
    )
    other = swap(other, (1, 1))
    (mine,) = call(4, mine_kernel, [shape((grads, cols), f32)], [], [tok_at], left, right, mine)
    return call(
        4, join_kernel,
        [shape((1, tag_count, cols), f32), shape((1, rank, cols), f32)], [], [], mine, other,
    )


def general(activations, pos_weight, depth_weight, tags, depths, counts):
    tag_count = pos_weight.shape[1]
    slots = tags.shape[0]
    rows = lax.all_to_all(activations, "layer", split_axis=0, concat_axis=1, tiled=True)[0]
    probe = jnp.concatenate([pos_weight[0], depth_weight[0]], axis=0)
    probe = lax.all_gather(probe, "tok", axis=1, tiled=True)
    scores = contract(rows, probe)
    logits, hidden = scores[:, :tag_count], scores[:, tag_count:]
    facts = jnp.stack([tags, depths, jnp.broadcast_to(counts, tags.shape)])
    tag_row, depth_row, block_count = lax.all_gather(facts, "layer", axis=1, tiled=True)
    live = jnp.arange(rows.shape[0], dtype=jnp.int32) % slots < block_count
    scale = jnp.where(live, 1.0 / block_count.astype(jnp.float32), jnp.float32(0.0))
    expo = jnp.exp(logits - jnp.max(logits, axis=1, keepdims=True))
    probabilities = expo / jnp.sum(expo, axis=1, keepdims=True)
    onehot = (tag_row[:, None] == jnp.arange(tag_count, dtype=jnp.int32)[None, :]).astype(jnp.float32)
    g_pos = (probabilities - onehot) * scale[:, None]
    predicted = jnp.sum(hidden * hidden, axis=1)
    g_depth = hidden * ((predicted - depth_row.astype(jnp.float32)) * scale)[:, None]
    joined = jnp.concatenate([g_pos, g_depth], axis=1).astype(jnp.bfloat16)
    share = lax.dot_general(
        joined, rows, (((0,), (0,)), ((), ())), preferred_element_type=jnp.float32
    )
    summed = lax.psum_scatter(share, "tok", scatter_dimension=1, tiled=True)
    return summed[None, :tag_count], summed[None, tag_count:]


def fits(layer_count, tok_count, activations, pos_weight, depth_weight):
    layers, slots, width = activations.shape
    cols = pos_weight.shape[2]
    grads = pos_weight.shape[1] + depth_weight.shape[1]
    return (
        layers == layer_count
        and layers >= 4
        and layers & (layers - 1) == 0
        and tok_count >= 4
        and tok_count & (tok_count - 1) == 0
        and cols % LANES == 0
        and width == cols * tok_count
        and slots % 4 == 0
        and slots >= 8
        and round_up((layers - 1) * slots, 8) + slots <= LANES
        and grads % 16 == 0
        and pos_weight.shape[1] % 16 == 0
    )


def local(activations, pos_weight, depth_weight, tags, depths, counts):
    sizes = lax.axis_size("layer"), lax.axis_size("tok")
    if fits(*sizes, activations, pos_weight, depth_weight):
        return fast(activations, pos_weight, depth_weight, tags, depths, counts)
    return general(activations, pos_weight, depth_weight, tags, depths, counts)


def solution(mesh):
    in_specs = (
        P(None, ("tok", "layer"), None),
        P("layer", None, "tok"),
        P("layer", None, "tok"),
        P(("tok", "layer")),
        P(("tok", "layer")),
        P(("tok", "layer")),
    )
    out_specs = (P("layer", None, "tok"), P("layer", None, "tok"))

    return jax.shard_map(local, mesh=mesh, in_specs=in_specs, out_specs=out_specs, check_vma=False)
```

```python
import functools

import jax
import jax.numpy as jnp
from jax import lax
from jax.experimental import pallas as pl
from jax.experimental.pallas import tpu as pltpu
from jax.sharding import PartitionSpec as P


LANES = 128


def contract(left, right):
    return lax.dot_general(
        left, right, (((1,), (1,)), ((), ())), preferred_element_type=jnp.float32
    )


def steps(count):
    width = count.bit_length() - 2
    chips = sorted(range(1, count // 2), key=lambda c: (-c.bit_count(), c))
    mirrored = [sum((c >> n & 1) << (width - 1 - n) for n in range(width)) for c in chips]
    return [(0, 0)] + [(2 * a, 2 * b) for a, b in zip(chips, mirrored)]


def peer(tok, step):
    first, second = step
    if isinstance(tok, int):
        return tok ^ (second if tok % 2 else first)
    return tok ^ jnp.where(tok % 2 == 0, first, second)


def swap(value, step):
    pairs = [(i, peer(i, step)) for i in range(lax.axis_size("tok"))]
    return lax.ppermute(value, "tok", pairs)


def gray(i):
    return i ^ (i >> 1)


def ungray(i, count):
    total = i
    for n in range(1, count.bit_length()):
        total = total ^ (i >> n)
    return total


def ring_shifts(count):
    return [1, count - 1] + list(range(2, count - 1))


def ring_target(i, shift, count):
    return gray((ungray(i, count) + shift) % count)


def spans(slots, pieces):
    base = slots // 8 * 8
    return [(p, 0, base) for p in range(pieces)] + [
        (p, base, slots) for p in range(pieces) if base < slots
    ]


def tile_rows(slots, lo, hi, tile):
    base = slots // 8 * 8
    start = tile // 2 * 2 * slots
    if lo < base:
        start += tile % 2 * base
    else:
        start += 2 * base + tile % 2 * (slots - base)
    return slice(start, start + hi - lo)


def round_up(value, step):
    return -(-value // step) * step


def pick_rows(held, target, out, slots, layers, tiles):
    base = slots // 8 * 8
    for t in tiles:
        rows = held[t, pl.ds(target, slots, stride=layers), :].astype(out.dtype)
        out[tile_rows(slots, 0, base, t), :] = rows[:base]
        if base < slots:
            out[tile_rows(slots, base, slots, t), :] = rows[base:]


def first_kernel(me, act, pos, depth, out, held, probe, raw, act_sems, sems, *, slots, layers):
    width = act.shape[2]
    parts = act_sems.shape[0]
    step = width // parts
    tag_count = pos.shape[1]
    loads = [
        pltpu.make_async_copy(
            act.at[:, :, pl.ds(n * step, step)], raw.at[:, :, pl.ds(n * step, step)], act_sems.at[n]
        )
        for n in range(parts)
    ]
    others = [
        pltpu.make_async_copy(pos.at[0], probe.at[:tag_count], sems.at[0]),
        pltpu.make_async_copy(depth.at[0], probe.at[tag_count:], sems.at[1]),
    ]
    for copy in loads + others:
        copy.start()
    target = ring_target(me[0], ring_shifts(layers)[0], layers)
    for n in range(parts):
        loads[n].wait()
        tiles = range(n * step // LANES, (n + 1) * step // LANES)
        for t in tiles:
            for s in range(slots):
                held[t, s * layers : (s + 1) * layers, :] = raw[
                    s, :, t * LANES : (t + 1) * LANES
                ].astype(jnp.float32)
        pick_rows(held, target, out, slots, layers, tiles)
    for copy in others:
        copy.wait()


def rest_kernel(me, held, *outs, slots, layers):
    targets = [me[0]] + [ring_target(me[0], s, layers) for s in ring_shifts(layers)[1:]]
    for target, out in zip(targets, outs):
        pick_rows(held, target, out, slots, layers, range(held.shape[0]))


def share_kernel(me, rows, probe, *outs, peers):
    grads, cols = probe.shape
    piece = outs[0].shape[0] - cols // LANES * grads
    for step, out in zip(peers, outs):
        out[:piece, :] = rows[pl.ds(chip_start(me[0], step, piece), piece), :]
        for t in range(cols // LANES):
            out[piece + t * grads : piece + (t + 1) * grads, :] = probe[
                :, t * LANES : (t + 1) * LANES
            ]


def cut_kernel(me, *refs, pieces, peers):
    parts, outs = refs[:pieces], refs[pieces:]
    piece = outs[0].shape[0] // pieces
    for step, out in zip(peers, outs):
        start = chip_start(me[0], step, piece)
        for n, part in enumerate(parts):
            out[n * piece : (n + 1) * piece, :] = part[pl.ds(start, piece), :]


def chip_start(tok, step, piece):
    return pl.multiple_of((peer(tok, step) // 2) * piece, 8)


def score_kernel(me, *refs, pieces, blocks, send, slots, tags, rank, peers):
    parts = refs[:pieces]
    probes = refs[pieces : pieces + len(blocks)]
    tokens = refs[pieces + len(blocks) : 2 * pieces + len(blocks)]
    outs, rows = refs[2 * pieces + len(blocks) : -1], refs[-1]
    grads = tags + rank
    tiles = rows.shape[1] // LANES
    tok_tiles = tiles // len(blocks)
    cols = tok_tiles * LANES
    piece = 2 * tok_tiles * slots
    order = spans(slots, pieces)
    at, facts = 0, []
    for p, lo, hi in order:
        for t in range(tiles):
            rows[at : at + hi - lo, t * LANES : (t + 1) * LANES] = parts[p][
                tile_rows(slots, lo, hi, t), :
            ]
        facts.append(tokens[p][:, lo:hi])
        at += hi - lo
    fact = jnp.concatenate(facts, axis=1)
    scores = None
    spots = [
        pl.ds(pl.multiple_of(peer(me[0] ^ flip, step) * cols, LANES), cols) for step, flip in blocks
    ]
    for n in range(0, len(blocks), 4):
        members = range(n, min(n + 4, len(blocks)))
        probe = jnp.concatenate(
            [
                probes[m][piece + t * grads : piece + (t + 1) * grads, :]
                for m in members
                for t in range(tok_tiles)
            ],
            axis=1,
        )
        part = contract(probe, jnp.concatenate([rows[:, spots[m]] for m in members], axis=1))
        scores = part if scores is None else scores + part
    logits, hidden = scores[:tags], scores[tags:]
    tag_row, depth_row, count_row, place = fact[0:1], fact[1:2], fact[2:3], fact[3:4]
    scale = jnp.where(place < count_row, 1.0 / count_row.astype(jnp.float32), jnp.float32(0.0))
    top = jnp.max(logits, axis=0, keepdims=True)
    expo = jnp.exp(logits - top)
    probabilities = expo / jnp.sum(expo, axis=0, keepdims=True)
    tag_at = lax.broadcasted_iota(jnp.int32, logits.shape, 0)
    onehot = (tag_at == tag_row).astype(jnp.float32)
    g_pos = (probabilities - onehot) * scale
    predicted = jnp.sum(hidden * hidden, axis=0, keepdims=True)
    g_depth = hidden * ((predicted - depth_row.astype(jnp.float32)) * scale)
    joined = jnp.concatenate([g_pos, g_depth], axis=0)
    folds = LANES // joined.shape[1]
    height = outs[0].shape[0] - piece
    if height * folds > grads:
        filler = jnp.zeros((height * folds - grads, joined.shape[1]), jnp.float32)
        joined = jnp.concatenate([joined, filler], axis=0)
    joined = jnp.concatenate([joined[n * height : (n + 1) * height] for n in range(folds)], axis=1)
    if joined.shape[1] < LANES:
        filler = jnp.zeros((height, LANES - joined.shape[1]), jnp.float32)
        joined = jnp.concatenate([joined, filler], axis=1)
    joined = joined.astype(jnp.bfloat16)
    for step, out in zip(peers, outs):
        out[:piece, :] = parts[send][pl.ds(chip_start(me[0], step, piece), piece), :]
        out[piece:, :] = joined


def fold_height(grads, tokens):
    folds = LANES // tokens
    return grads if folds == 1 else round_up(-(-grads // folds), 16)


def gather_rows(right, at, sources, slots, tiles):
    for p, lo, hi in spans(slots, len(sources)):
        for t in range(tiles):
            right[at : at + hi - lo, t * LANES : (t + 1) * LANES] = sources[p][
                tile_rows(slots, lo, hi, t), :
            ]
        at += hi - lo
    return at


def stage_kernel(me, *refs, chips, slots, sets):
    messages = [refs[n * chips : (n + 1) * chips] for n in range(sets)]
    mine, other, left, right = refs[sets * chips :]
    cols = mine.shape[1]
    tiles = 2 * cols // LANES
    for c in range(chips):
        at, stop = c * LANES, (c + 1) * LANES
        left[:, at:stop] = messages[1][c][tiles * slots :, :]
        at = gather_rows(right, at, [part[c] for part in messages], slots, tiles)
        if at < stop:
            right[at:stop, :] = jnp.zeros((stop - at, 2 * cols), right.dtype)
    core = me[0] % 2
    mine[...] = half_grad(left, right, core, cols)
    other[...] = half_grad(left, right, 1 - core, cols)


def grad_kernel(me, *refs, chips, slots):
    lates, so_far = refs[:chips], refs[chips]
    other, left, right = refs[chips + 1 :]
    grads, cols = other.shape
    tiles = 2 * cols // LANES
    pad = right.shape[0] // chips
    folds = LANES // slots
    parts = []
    for c in range(chips):
        tail = lates[c][tiles * slots :, :].astype(jnp.float32)
        tail = jnp.concatenate([tail[:, n * slots : (n + 1) * slots] for n in range(folds)], axis=0)
        parts.append(tail[:grads])
        at, stop = c * pad, (c + 1) * pad
        if slots < pad:
            parts.append(jnp.zeros((grads, pad - slots), jnp.float32))
        at = gather_rows(right, at, [lates[c]], slots, tiles)
        if at < stop:
            right[at:stop, :] = jnp.zeros((stop - at, 2 * cols), right.dtype)
    left[...] = jnp.concatenate(parts, axis=1).astype(left.dtype)
    half = half_grad(left, right, 1 - me[0] % 2, cols)
    other[...] = (so_far[...] + half).astype(other.dtype)


def half_grad(left, right, half, cols):
    spot = pl.ds(pl.multiple_of(half * cols, LANES), cols)
    return jnp.dot(left[...], right[:, spot], preferred_element_type=jnp.float32)


def mine_kernel(me, left, right, so_far, mine):
    mine[...] = so_far[...] + half_grad(left, right, me[0] % 2, mine.shape[1])


def join_kernel(mine, other, pos_out, depth_out, held, sems):
    tags, rank = pos_out.shape[1], depth_out.shape[1]
    half = rank // 2
    parts = [
        (0, tags, pos_out.at[0]),
        (tags, tags + half, depth_out.at[0, :half]),
        (tags + half, tags + rank, depth_out.at[0, half:]),
    ]
    copies = []
    for n, (lo, hi, target) in enumerate(parts):
        held[lo:hi, :] = mine[lo:hi, :] + other[lo:hi, :].astype(jnp.float32)
        copies.append(pltpu.make_async_copy(held.at[lo:hi], target, sems.at[n]))
        copies[-1].start()
    for copy in copies:
        copy.wait()


def call(vmem, kernel, outs, scratch, scalars, *values, spaces=()):
    local = pl.BlockSpec(memory_space=pltpu.VMEM)
    specs = [pl.BlockSpec(memory_space=pltpu.SMEM)] * len(scalars)
    specs += [pl.BlockSpec(memory_space=s) for s in spaces]
    specs += [local] * (len(values) - len(spaces))
    return pl.pallas_call(
        kernel,
        out_shape=outs,
        in_specs=specs,
        out_specs=[local] * len(outs),
        scratch_shapes=scratch,
        compiler_params=pltpu.CompilerParams(vmem_limit_bytes=vmem << 20),
    )(*scalars, *values)


def fast(activations, pos_weight, depth_weight, tags, depths, counts):
    layer_count, tok_count = lax.axis_size("layer"), lax.axis_size("tok")
    tag_count, cols = pos_weight.shape[1:]
    rank = depth_weight.shape[1]
    slots = tags.shape[0]
    layers, _, width = activations.shape
    bf16, f32, i32 = jnp.bfloat16, jnp.float32, jnp.int32
    shape = jax.ShapeDtypeStruct
    grads = tag_count + rank
    layer_at = lax.axis_index("layer").astype(i32)[None]
    tok_at = lax.axis_index("tok").astype(i32)[None]
    peers = steps(tok_count)
    piece = 2 * cols // LANES * slots

    def exchange(values):
        return [values[0]] + [swap(v, step) for step, v in zip(peers[1:], values[1:])]

    message = shape((width // LANES * slots, LANES), bf16)
    held_shape = (width // LANES, slots * layers, LANES)
    shifts = ring_shifts(layer_count)

    def along(value, shift):
        pairs = [(i, ring_target(i, shift, layer_count)) for i in range(layer_count)]
        return lax.ppermute(value, "layer", pairs)

    head, held, probe = call(
        12, functools.partial(first_kernel, slots=slots, layers=layers),
        [message, shape(held_shape, f32), shape((grads, cols), bf16)],
        [
            pltpu.VMEM((slots, layers, width), bf16),
            pltpu.SemaphoreType.DMA((4,)),
            pltpu.SemaphoreType.DMA((2,)),
        ],
        [layer_at],
        *[
            pltpu.with_memory_space_constraint(v, pltpu.HBM)
            for v in (jnp.transpose(activations, (1, 0, 2)), pos_weight, depth_weight)
        ],
        spaces=[pltpu.HBM] * 3,
    )
    own, *others = call(
        4, functools.partial(rest_kernel, slots=slots, layers=layers),
        [message] * (layers - 1), [], [layer_at], held,
    )
    pieces = [own] + [along(v, shift) for v, shift in zip([head] + others, shifts)]
    fact = jnp.stack([tags, depths, jnp.broadcast_to(counts, tags.shape), jnp.arange(slots, dtype=i32)])
    facts = [fact] + [along(fact, shift) for shift in shifts]
    shares = call(
        4, functools.partial(share_kernel, peers=peers),
        [shape((piece + cols // LANES * grads, LANES), bf16)] * len(peers),
        [], [tok_at], own, probe,
    )
    shares = exchange(shares)
    probes = shares + [swap(v, (1, 1)) for v in shares]
    blocks = [(step, 0) for step in peers] + [(step, 1) for step in peers]
    early = [
        exchange(
            call(
                4, functools.partial(cut_kernel, pieces=1, peers=peers),
                [shape((piece, LANES), bf16)] * len(peers), [], [tok_at], pieces[n],
            ),
        )
        for n in range(2, layers - 1)
    ]

    def score(members, send):
        outs = call(
            12,
            functools.partial(
                score_kernel, pieces=len(members), blocks=blocks, send=send, slots=slots,
                tags=tag_count, rank=rank, peers=peers,
            ),
            [shape((piece + fold_height(grads, len(members) * slots), LANES), bf16)] * len(peers),
            [pltpu.VMEM((len(members) * slots, width), bf16)],
            [tok_at], *[pieces[n] for n in members], *probes, *[facts[n] for n in members],
        )
        return exchange(outs)

    middle = score(range(layers - 1), 1)
    late = score([layers - 1], 0)
    part = shape((grads, cols), f32)
    count = len(peers)
    mine, other = call(
        8, functools.partial(stage_kernel, chips=count, slots=slots, sets=layers - 1),
        [part, part],
        [pltpu.VMEM((grads, count * LANES), bf16), pltpu.VMEM((count * LANES, 2 * cols), bf16)],
        [tok_at], *shares, *middle, *[v for values in early for v in values],
    )
    depth = count * round_up(slots, 16)
    other, left, right = call(
        8, functools.partial(grad_kernel, chips=count, slots=slots),
        [shape((grads, cols), bf16), shape((grads, depth), bf16), shape((depth, 2 * cols), bf16)],
        [], [tok_at], *late, other,
    )
    other = swap(other, (1, 1))
    (mine,) = call(4, mine_kernel, [shape((grads, cols), f32)], [], [tok_at], left, right, mine)
    local_space, far = pl.BlockSpec(memory_space=pltpu.VMEM), pl.BlockSpec(memory_space=pltpu.HBM)
    return pl.pallas_call(
        join_kernel,
        out_shape=[shape((1, tag_count, cols), f32), shape((1, rank, cols), f32)],
        in_specs=[local_space] * 2,
        out_specs=[far] * 2,
        scratch_shapes=[pltpu.VMEM((grads, cols), f32), pltpu.SemaphoreType.DMA((3,))],
        compiler_params=pltpu.CompilerParams(vmem_limit_bytes=4 << 20),
        name="join",
    )(mine, other)


def general(activations, pos_weight, depth_weight, tags, depths, counts):
    tag_count = pos_weight.shape[1]
    slots = tags.shape[0]
    rows = lax.all_to_all(activations, "layer", split_axis=0, concat_axis=1, tiled=True)[0]
    probe = jnp.concatenate([pos_weight[0], depth_weight[0]], axis=0)
    probe = lax.all_gather(probe, "tok", axis=1, tiled=True)
    scores = contract(rows, probe)
    logits, hidden = scores[:, :tag_count], scores[:, tag_count:]
    facts = jnp.stack([tags, depths, jnp.broadcast_to(counts, tags.shape)])
    tag_row, depth_row, block_count = lax.all_gather(facts, "layer", axis=1, tiled=True)
    live = jnp.arange(rows.shape[0], dtype=jnp.int32) % slots < block_count
    scale = jnp.where(live, 1.0 / block_count.astype(jnp.float32), jnp.float32(0.0))
    expo = jnp.exp(logits - jnp.max(logits, axis=1, keepdims=True))
    probabilities = expo / jnp.sum(expo, axis=1, keepdims=True)
    onehot = (tag_row[:, None] == jnp.arange(tag_count, dtype=jnp.int32)[None, :]).astype(jnp.float32)
    g_pos = (probabilities - onehot) * scale[:, None]
    predicted = jnp.sum(hidden * hidden, axis=1)
    g_depth = hidden * ((predicted - depth_row.astype(jnp.float32)) * scale)[:, None]
    joined = jnp.concatenate([g_pos, g_depth], axis=1).astype(jnp.bfloat16)
    share = lax.dot_general(
        joined, rows, (((0,), (0,)), ((), ())), preferred_element_type=jnp.float32
    )
    summed = lax.psum_scatter(share, "tok", scatter_dimension=1, tiled=True)
    return summed[None, :tag_count], summed[None, tag_count:]


def fits(layer_count, tok_count, activations, pos_weight, depth_weight):
    layers, slots, width = activations.shape
    cols = pos_weight.shape[2]
    grads = pos_weight.shape[1] + depth_weight.shape[1]
    return (
        layers == layer_count
        and layers >= 4
        and layers & (layers - 1) == 0
        and tok_count >= 4
        and tok_count & (tok_count - 1) == 0
        and cols % LANES == 0
        and width == cols * tok_count
        and slots % 4 == 0
        and slots >= 8
        and round_up((layers - 1) * slots, 8) + slots <= LANES
        and grads % 16 == 0
        and pos_weight.shape[1] % 16 == 0
    )


def local(activations, pos_weight, depth_weight, tags, depths, counts):
    sizes = lax.axis_size("layer"), lax.axis_size("tok")
    if fits(*sizes, activations, pos_weight, depth_weight):
        return fast(activations, pos_weight, depth_weight, tags, depths, counts)
    return general(activations, pos_weight, depth_weight, tags, depths, counts)


def solution(mesh):
    in_specs = (
        P(None, ("tok", "layer"), None),
        P("layer", None, "tok"),
        P("layer", None, "tok"),
        P(("tok", "layer")),
        P(("tok", "layer")),
        P(("tok", "layer")),
    )
    out_specs = (P("layer", None, "tok"), P("layer", None, "tok"))

    return jax.shard_map(local, mesh=mesh, in_specs=in_specs, out_specs=out_specs, check_vma=False)
```
